32 devices in a mesh: dp: 4 (over x, core), section: 2 (over y), mp: 4 (over z).
Axes of the slice: x: 2, y: 2, z: 4, core: 2. Of those that a mesh axis runs over, the one named last changes fastest.
Arguments:
- micro_inputs: bfloat16 [8, 64, 4096], P(('dp', 'section'), None, 'mp'), parts along dimension 0, may hold values from -6 to 6
- qkv_weight: bfloat16 [2, 4096, 3, 2048], P('section', None, None, 'mp'), may hold values from -0.09375 to 0.09375
- out_weight: bfloat16 [2, 2048, 4096], P('section', None, 'mp'), may hold values from -0.125 to 0.125
- norm_gain: bfloat16 [2, 4096], P('section'), may hold values from 0.099609375 to 1.8984375
- position_bias: float32 [32, 32], P('mp'), may hold values from -3 to 280
Outputs:
- encoded: bfloat16 [8, 64, 4096], P(('dp', 'section'), None, 'mp'), parts along dimension 0
The draws below stay inside these ranges and needn't reach their ends.
There are 4 independent parts, one for each index of `dp`. The reference program is written for one: setup_inputs(seed, part) draws one part's arguments, and reference() takes and returns one part's arrays. A program takes and returns all parts, laid end to end along the dimension named above; an argument that names none is the same for every part. Nothing has to cross between parts.
All inputs are finite; a program needn't handle non-finite values.
Results may differ from the reference program's by a relative error of at most 0.025.
Values may be sent and summed in bfloat16 or wider, within the bound.
No kernel may reach another device: no remote copies, remote signals or barrier semaphores. Data moves between devices by JAX's collectives and lax.ppermute only.
A program may use at most 128 MiB of HBM per device.

```python
import math
import jax
import jax.numpy as jnp
import numpy as np
from jax import lax

D = 4096
HS = 64
HEADS = 32
BUCKETS = 32
REACH = 128
LENGTH = 64
LAYERS = 2
MICROS = 2


def draw_position_bias(key, part):
    ordinary = jnp.clip(jax.random.normal(key, (HEADS, BUCKETS), jnp.float32), -3.0, 3.0)
    return ordinary


def shard_levels(rng, dims, shards, smallest, largest):
    def one(position, parts):
        steps = jax.random.uniform(jax.random.fold_in(jax.random.fold_in(rng, 6), position), (parts,), jnp.float32, smallest / len(shards), largest / len(shards))
        return jnp.repeat(jnp.exp(steps), dims[position] // parts).reshape((-1,) + (1,) * (len(dims) - position - 1))

    level = one(*shards[0])
    for cut in shards[1:]:
        level = level * one(*cut)
    return level


def centred(rng, shape, scale, most, split=(), kind=jnp.bfloat16):
    values = scale * jax.random.normal(rng, shape, jnp.float32)
    if split:
        values = values * shard_levels(rng, shape, split, -0.22, 0.18)
    return jnp.clip(values, -most, most).astype(kind)


def setup_inputs(seed: int = 0, part: int = 0) -> dict:
    seeds = jax.random.split(jax.random.key(seed), 6)
    own_keys = jax.random.split(jax.random.fold_in(seeds[5], part), 6)
    micro_inputs = centred(own_keys[0], (MICROS, LENGTH, D), 1.0, 6.0, ((0, 2), (2, 4)))
    qkv_weight = centred(seeds[1], (LAYERS, D, 3, HEADS * HS), D ** -0.5, 0.09375, ((0, 2), (3, 4)))
    out_weight = centred(seeds[2], (LAYERS, HEADS * HS, D), (HEADS * HS) ** -0.5, 0.125, ((0, 2), (2, 4)))
    norm_gain = jnp.clip(1.0 + 0.18 * jax.random.normal(seeds[3], (LAYERS, D), jnp.float32), 0.099609375, 1.8984375).astype(jnp.bfloat16)
    position_bias = draw_position_bias(jax.random.fold_in(seeds[5], 71), part)
    return {"micro_inputs": micro_inputs, "qkv_weight": qkv_weight, "out_weight": out_weight, "norm_gain": norm_gain, "position_bias": position_bias}


NORM_EPSILON = 0.1

def bucket_table(length, bucket_count, reach_limit):
    offset = np.arange(length)[None, :] - np.arange(length)[:, None]
    half_count = bucket_count // 2
    upper_side = (offset > 0).astype(np.int32) * half_count
    distance = np.abs(offset)
    exact_count = half_count // 2
    scaled = np.log(np.maximum(distance, 1) / exact_count) / np.log(reach_limit / exact_count) * (half_count - exact_count)
    far_bucket = np.minimum(exact_count + scaled.astype(np.int32), half_count - 1)
    return (upper_side + np.where(distance < exact_count, distance, far_bucket)).astype(np.int32)

def reference(micro_inputs, qkv_weight, out_weight, norm_gain, position_bias):
    bucket_grid = jnp.asarray(bucket_table(LENGTH, BUCKETS, REACH)).astype(jnp.int32)
    score_bias = position_bias[:, bucket_grid].astype(jnp.float32)
    score_scale = 1.0 / math.sqrt(HS)

    def layer_step(hidden, layer_index):
        stream = hidden.astype(jnp.float32)
        mean_square = lax.optimization_barrier(jnp.mean(stream * stream, axis=1, keepdims=True))
        row_scale = lax.rsqrt(mean_square + NORM_EPSILON)
        gained = (stream * norm_gain[layer_index].astype(jnp.float32)).astype(jnp.bfloat16)
        weight_grid = qkv_weight[layer_index].reshape(D, 3 * HEADS * HS)
        project = jnp.dot(gained, weight_grid, preferred_element_type=jnp.float32) * row_scale
        rounded = lax.optimization_barrier(project.astype(jnp.bfloat16))
        project = rounded.astype(jnp.float32).reshape(LENGTH, 3, HEADS, HS)
        queries = project[:, 0]
        key_heads = project[:, 1]
        values = project[:, 2]
        scores = jnp.einsum('ihd,jhd->hij', queries, key_heads, precision=lax.Precision.HIGHEST) * score_scale + score_bias
        row_max = lax.optimization_barrier(jnp.max(scores, axis=2, keepdims=True))
        weights = jnp.exp(scores - row_max)
        attn_probs = lax.optimization_barrier((weights / lax.optimization_barrier(jnp.sum(weights, axis=2, keepdims=True))).astype(jnp.bfloat16))
        head_mix = jnp.einsum('hij,jhd->ihd', attn_probs.astype(jnp.float32), values, precision=lax.Precision.HIGHEST)
        head_mix = head_mix.astype(jnp.bfloat16).reshape(LENGTH, HEADS * HS)
        update = jnp.dot(head_mix, out_weight[layer_index], preferred_element_type=jnp.float32)
        return ((stream + update).astype(jnp.bfloat16), None)

    def run_micro(micro_rows):
        finished, unused = lax.scan(layer_step, micro_rows, jnp.arange(LAYERS, dtype=jnp.int32))
        return finished
    return lax.map(run_micro, micro_inputs)
```

```python
import math

import jax
import jax.numpy as jnp
import numpy as np
from jax import lax
from jax.sharding import PartitionSpec as P

REACH = 128
NORM_EPSILON = 0.1
MOST_DIRECT = 4


def bucket_table(length, bucket_count, reach_limit):
    offset = np.arange(length)[None, :] - np.arange(length)[:, None]
    half_count = bucket_count // 2
    upper_side = (offset > 0).astype(np.int32) * half_count
    distance = np.abs(offset)
    exact_count = half_count // 2
    scaled = (
        np.log(np.maximum(distance, 1) / exact_count)
        / np.log(reach_limit / exact_count)
        * (half_count - exact_count)
    )
    far_bucket = np.minimum(exact_count + scaled.astype(np.int32), half_count - 1)
    return (upper_side + np.where(distance < exact_count, distance, far_bucket)).astype(np.int32)


def swap_orders(peers):
    return sorted(range(1, peers), key=lambda mask: (bin(mask).count("1"), mask))


def pieces(x, axis):
    peers = lax.axis_size(axis)
    me = lax.axis_index(axis)
    if peers & (peers - 1) or peers > MOST_DIRECT:
        whole = lax.all_gather(x, axis, axis=0, tiled=False)
        return [(p, whole[p]) for p in range(peers)]
    got = [(me, x)]
    for mask in swap_orders(peers):
        other = lax.ppermute(x, axis, [(i, i ^ mask) for i in range(peers)])
        got.append((me ^ mask, other))
    return got


def shards(micro_inputs, qkv_weight, out_weight, norm_gain, position_bias):
    sections = lax.axis_size("section")
    section_index = lax.axis_index("section")
    length = micro_inputs.shape[1]
    local_width = micro_inputs.shape[2]
    model_width = qkv_weight.shape[1]
    local_heads = position_bias.shape[0]
    local_qkv = qkv_weight.shape[3]
    head_size = local_qkv // local_heads
    peers = lax.axis_size("mp")
    weights_qkv = jnp.transpose(qkv_weight[0], (1, 0, 2))
    weights_out = out_weight[0]
    gain_row = norm_gain[0].astype(jnp.float32)
    bucket_count = position_bias.shape[1]
    bucket_grid = jnp.asarray(bucket_table(length, bucket_count, REACH))
    onehot = (
        bucket_grid[:, :, None] == jnp.arange(bucket_count, dtype=jnp.int32)[None, None, :]
    ).astype(jnp.float32)
    score_bias = jnp.einsum("hb,ijb->hij", position_bias, onehot, precision=lax.Precision.HIGHEST)
    score_scale = 1.0 / math.sqrt(head_size)

    def attend(section_in):
        stream = section_in.astype(jnp.float32)
        project = jnp.zeros((3, length, local_qkv), jnp.float32)
        squares = jnp.zeros((length,), jnp.float32)
        for peer, block in pieces(section_in, "mp"):
            rows = block.astype(jnp.float32)
            squares = squares + jnp.sum(rows * rows, axis=1)
            start = peer * local_width
            gain = lax.dynamic_slice_in_dim(gain_row, start, local_width, 0)
            part = lax.dynamic_slice_in_dim(weights_qkv, start, local_width, 1)
            gained = (rows * gain).astype(jnp.bfloat16)
            project = project + jnp.einsum(
                "cik,ckn->cin",
                jnp.broadcast_to(gained, (3,) + gained.shape),
                part,
                preferred_element_type=jnp.float32,
            )
        row_scale = lax.rsqrt(squares / model_width + NORM_EPSILON)[:, None]
        project = (project * row_scale).astype(jnp.bfloat16)
        project = project.reshape(3, length, local_heads, head_size)
        queries, key_heads, values = project[0], project[1], project[2]
        scores = (
            jnp.einsum("ihd,jhd->hij", queries, key_heads, preferred_element_type=jnp.float32)
            * score_scale
            + score_bias
        )
        row_max = jnp.max(scores, axis=2, keepdims=True)
        weights = jnp.exp(scores - row_max)
        attn_probs = (weights / jnp.sum(weights, axis=2, keepdims=True)).astype(jnp.bfloat16)
        head_mix = jnp.einsum(
            "hij,jhd->ihd", attn_probs, values, preferred_element_type=jnp.float32
        )
        head_mix = head_mix.astype(jnp.bfloat16).reshape(length, local_qkv)
        update = stream
        for peer, block in pieces(head_mix, "mp"):
            part = lax.dynamic_slice_in_dim(weights_out, peer * local_qkv, local_qkv, 0)
            update = update + jnp.dot(block, part, preferred_element_type=jnp.float32)
        return update.astype(jnp.bfloat16)

    def rotated(x, by):
        pairs = [(i, (i + by) % sections) for i in range(sections)]
        return lax.ppermute(x, "section", pairs)

    first = section_index == 0
    raw = micro_inputs[0]
    ticks = 2 * sections - 1
    current = raw
    result = raw
    for tick in range(ticks):
        if tick + 1 < sections:
            raw = rotated(raw, -1)
        out = attend(current)
        finished = tick - (sections - 1)
        if tick + 1 < ticks:
            sent = rotated(out, 1)
            current = jnp.where(first, raw, sent)
        if finished >= 0:
            owned = rotated(out, finished + 1) if tick + 1 < ticks and finished else (
                sent if tick + 1 < ticks else out)
            result = jnp.where(section_index == finished, owned, result)
    return result[None]


def solution(mesh):
    in_specs = (
        P(("dp", "section"), None, "mp"),
        P("section", None, None, "mp"),
        P("section", None, "mp"),
        P("section", None),
        P("mp", None),
    )
    out_specs = P(("dp", "section"), None, "mp")
    return jax.shard_map(shards, mesh=mesh, in_specs=in_specs, out_specs=out_specs, check_vma=False)
```

```python
import math

import jax
import jax.numpy as jnp
import numpy as np
from jax import lax
from jax.experimental import pallas as pl
from jax.experimental.pallas import tpu as pltpu
from jax.sharding import PartitionSpec as P

REACH = 128
NORM_EPSILON = 0.1
MOST_DIRECT = 4
LANES = 128
F32 = jnp.float32
BF16 = jnp.bfloat16
VMEM = pltpu.VMEM


def bucket_table(length, bucket_count, reach_limit):
    offset = np.arange(length)[None, :] - np.arange(length)[:, None]
    half_count = bucket_count // 2
    upper_side = (offset > 0).astype(np.int32) * half_count
    distance = np.abs(offset)
    exact_count = half_count // 2
    scaled = (
        np.log(np.maximum(distance, 1) / exact_count)
        / np.log(reach_limit / exact_count)
        * (half_count - exact_count)
    )
    far_bucket = np.minimum(exact_count + scaled.astype(np.int32), half_count - 1)
    return (upper_side + np.where(distance < exact_count, distance, far_bucket)).astype(np.int32)


def swap_masks(peers):
    if peers & (peers - 1) or peers > MOST_DIRECT:
        return None
    return sorted(range(1, peers), key=lambda mask: (bin(mask).count("1"), mask))


def from_peers(x, axis):
    peers = lax.axis_size(axis)
    masks = swap_masks(peers)
    if masks is None:
        return [lax.all_gather(x, axis, axis=0, tiled=False)]
    return [lax.ppermute(x, axis, [(i, i ^ mask) for i in range(peers)]) for mask in masks]


def peer_blocks(refs, axis):
    peers = lax.axis_size(axis)
    me = lax.axis_index(axis)
    masks = swap_masks(peers)
    if masks is None:
        turned = [lax.rem(me + step, peers) for step in range(1, peers)]
        return [(peer, refs[0][peer]) for peer in turned]
    return [(me ^ mask, ref[...]) for mask, ref in zip(masks, refs)]


def rows_of(peer, count):
    return pl.ds(pl.multiple_of(peer * count, count), count)


def call(body, outs, *args, specs=None, scratch=(), limit=8):
    specs = specs or [pl.BlockSpec(memory_space=VMEM)] * len(args)
    return pl.pallas_call(
        body,
        in_specs=specs,
        out_specs=tuple(pl.BlockSpec(memory_space=VMEM) for _ in outs),
        out_shape=tuple(outs),
        scratch_shapes=list(scratch),
        compiler_params=pltpu.CompilerParams(vmem_limit_bytes=limit << 20),
    )(*args)


def add_part(peer, block, gain_ref, weight_ref, total_ref, squares):
    width = block.shape[1]
    rows = block.astype(F32)
    gain = gain_ref[:, rows_of(peer, width)].astype(F32)
    gained = (rows * gain).astype(BF16)
    for lane in range(0, width, LANES):
        tile = rows[:, lane : lane + LANES]
        squares = squares + tile * tile
    for kind in range(weight_ref.shape[0]):
        part = weight_ref[kind, rows_of(peer, width), :]
        total_ref[kind] += jnp.dot(gained, part, preferred_element_type=F32)
    return squares


def own_part(peer, block, gain_ref, weight_ref, total_ref, squares_ref):
    total_ref[...] = jnp.zeros_like(total_ref)
    squares = jnp.zeros(squares_ref.shape, F32)
    squares_ref[...] = add_part(peer, block, gain_ref, weight_ref, total_ref, squares)


def load_kernel(x_ref, gain_ref, qkv_ref, out_ref, table_ref, grid_ref,
                held_qkv, held_out, total_ref, squares_ref, bias_ref, sems):
    peers = lax.axis_size("mp")
    me = lax.axis_index("mp")
    width = x_ref.shape[1]
    copies = []
    for step in range(peers):
        rows = rows_of(lax.rem(me + step, peers), width)
        copies.append(pltpu.make_async_copy(
            qkv_ref.at[:, rows, :], held_qkv.at[:, rows, :], sems.at[step]))
    copies.append(pltpu.make_async_copy(out_ref, held_out, sems.at[peers]))
    for copy in copies:
        copy.start()
    heads, buckets = table_ref.shape
    length = grid_ref.shape[0]

    def one_head(head, carry):
        grid = grid_ref[...]
        bias = jnp.zeros(grid.shape, F32)
        for bucket in range(buckets):
            bias = jnp.where(grid == bucket, table_ref[head, bucket], bias)
        bias_ref[rows_of(head, length), :] = bias
        return carry

    lax.fori_loop(0, heads, one_head, 0)
    copies[0].wait()
    own_part(me, x_ref[...], gain_ref, held_qkv, total_ref, squares_ref)
    for copy in copies[1:]:
        copy.wait()


def own_kernel(x_ref, gain_ref, held_qkv, total_ref, squares_ref):
    own_part(lax.axis_index("mp"), x_ref[...], gain_ref, held_qkv, total_ref, squares_ref)


def attend_kernel(head_size, model_width, *refs):
    *peer_refs, gain_ref, held_qkv, partial_ref, partial_squares, bias_ref, mix_ref, total_ref = refs
    total_ref[...] = partial_ref[...]
    squares = partial_squares[...]
    for peer, block in peer_blocks(peer_refs, "mp"):
        squares = add_part(peer, block, gain_ref, held_qkv, total_ref, squares)
    mean_square = jnp.sum(squares, axis=1, keepdims=True) / model_width
    row_scale = lax.rsqrt(mean_square + NORM_EPSILON)
    length, local_qkv = mix_ref.shape
    score_scale = 1.0 / math.sqrt(head_size)
    block_heads = LANES // head_size
    lane = lax.broadcasted_iota(jnp.int32, (length, LANES), 1) // head_size
    for block in range(local_qkv // LANES):
        lanes = pl.ds(block * LANES, LANES)
        queries, keys, values = (total_ref[kind, :, lanes] * row_scale for kind in range(3))
        keys = keys.astype(BF16)
        values = values.astype(BF16)
        stacked = jnp.concatenate(
            [jnp.where(lane == head, queries, 0.0) for head in range(block_heads)], axis=0
        ).astype(BF16)
        scores = lax.dot_general(
            stacked, keys, (((1,), (1,)), ((), ())), preferred_element_type=F32)
        rows = pl.ds(block * block_heads * length, block_heads * length)
        scores = scores * score_scale + bias_ref[rows, :]
        weights = jnp.exp(scores - jnp.max(scores, axis=1, keepdims=True))
        probs = (weights / jnp.sum(weights, axis=1, keepdims=True)).astype(BF16)
        mixed = jnp.dot(probs, values, preferred_element_type=F32)
        mix = mixed[:length]
        for head in range(1, block_heads):
            mix = jnp.where(lane == head, mixed[head * length : (head + 1) * length], mix)
        mix_ref[:, lanes] = mix.astype(BF16)


def out_kernel(keep_section, *refs):
    *peer_refs, own_ref, held_out, stream_ref, kept_ref, result_ref = refs
    local_qkv = own_ref.shape[1]
    total = stream_ref[...].astype(F32)
    blocks = [(lax.axis_index("mp"), own_ref[...])] + peer_blocks(peer_refs, "mp")
    for peer, block in blocks:
        part = held_out[rows_of(peer, local_qkv), :]
        total += jnp.dot(block, part, preferred_element_type=F32)
    result = total.astype(BF16)
    if keep_section is not None:
        result = jnp.where(lax.axis_index("section") == keep_section, kept_ref[...], result)
    result_ref[...] = result


def pick_kernel(section, a_ref, b_ref, o_ref):
    o_ref[...] = jnp.where(lax.axis_index("section") == section, a_ref[...], b_ref[...])


def pick(section, a, b):
    return call(lambda *refs: pick_kernel(section, *refs), [VMEM(a.shape, a.dtype)], a, b)[0]


def shards(micro_inputs, qkv_weight, out_weight, norm_gain, position_bias):
    sections = lax.axis_size("section")
    peers = lax.axis_size("mp")
    length = micro_inputs.shape[1]
    model_width = qkv_weight.shape[1]
    local_heads, bucket_count = position_bias.shape
    local_qkv = qkv_weight.shape[3]
    head_size = local_qkv // local_heads
    weights_qkv = jnp.transpose(qkv_weight[0], (1, 0, 2))
    weights_out = out_weight[0]
    bucket_grid = jnp.asarray(bucket_table(length, bucket_count, REACH))

    total = VMEM((3, length, local_qkv), F32)
    squares = VMEM((length, LANES), F32)
    held = {}

    def attend(section_in, keep_section, kept):
        others = from_peers(section_in, "mp")
        if not held:
            vm = pl.BlockSpec(memory_space=VMEM)
            hbm = pl.BlockSpec(memory_space=pltpu.HBM)
            sm = pl.BlockSpec(memory_space=pltpu.SMEM)
            bias = VMEM((local_heads * length, length), F32)
            held["qkv"], held["out"], part, part_squares, held["bias"] = call(
                load_kernel,
                [VMEM(weights_qkv.shape, BF16), VMEM(weights_out.shape, BF16), total, squares, bias],
                section_in, norm_gain, weights_qkv, weights_out, position_bias, bucket_grid,
                specs=[vm, vm, hbm, hbm, sm, vm],
                scratch=[pltpu.SemaphoreType.DMA((peers + 1,))],
            )
        else:
            part, part_squares = call(
                own_kernel, [total, squares], section_in, norm_gain, held["qkv"])
        mix = call(
            lambda *refs: attend_kernel(head_size, model_width, *refs),
            [VMEM((length, local_qkv), BF16)],
            *others, norm_gain, held["qkv"], part, part_squares, held["bias"],
            scratch=[total],
        )[0]
        mixes = from_peers(mix, "mp")
        return call(
            lambda *refs: out_kernel(keep_section, *refs),
            [VMEM(section_in.shape, BF16)],
            *mixes, mix, held["out"], section_in, kept,
        )[0]

    def rotated(x, by):
        return lax.ppermute(x, "section", [(i, (i + by) % sections) for i in range(sections)])

    raw = micro_inputs[0]
    if sections == 2:
        handed = rotated(attend(raw, 1, raw), 1)
        finished = rotated(attend(handed, None, raw), 1)
        return attend(finished, 0, finished)[None]
    ticks = 2 * sections - 1
    current = raw
    result = raw
    for tick in range(ticks):
        if tick + 1 < sections:
            raw = rotated(raw, -1)
        out = attend(current, None, current)
        done = tick - (sections - 1)
        if tick + 1 < ticks:
            sent = rotated(out, 1)
            current = pick(0, raw, sent)
        if done >= 0:
            owned = rotated(out, done + 1) if done + 1 < sections else out
            result = pick(done, owned, result)
    return result[None]


def solution(mesh):
    in_specs = (
        P(("dp", "section"), None, "mp"),
        P("section", None, None, "mp"),
        P("section", None, "mp"),
        P("section", None),
        P("mp", None),
    )
    out_specs = P(("dp", "section"), None, "mp")
    return jax.shard_map(shards, mesh=mesh, in_specs=in_specs, out_specs=out_specs, check_vma=False)
```

```python
import math

import jax
import jax.numpy as jnp
import numpy as np
from jax import lax
from jax.experimental import pallas as pl
from jax.experimental.pallas import tpu as pltpu
from jax.sharding import PartitionSpec as P

REACH = 128
NORM_EPSILON = 0.1
MOST_DIRECT = 4
FIRST_ORDER = (1, 3, 2)
MIX_ORDER = (1, 3, 2)
REST_ORDER = (1, 3, 2)
ACROSS = (2,)
LANES = 128
F32 = jnp.float32
BF16 = jnp.bfloat16
VMEM = pltpu.VMEM


def bucket_table(length, bucket_count, reach_limit):
    offset = np.arange(length)[None, :] - np.arange(length)[:, None]
    half_count = bucket_count // 2
    upper_side = (offset > 0).astype(np.int32) * half_count
    distance = np.abs(offset)
    exact_count = half_count // 2
    scaled = (
        np.log(np.maximum(distance, 1) / exact_count)
        / np.log(reach_limit / exact_count)
        * (half_count - exact_count)
    )
    far_bucket = np.minimum(exact_count + scaled.astype(np.int32), half_count - 1)
    return (upper_side + np.where(distance < exact_count, distance, far_bucket)).astype(np.int32)


def swap_masks(peers, order=MIX_ORDER):
    if peers & (peers - 1) or peers > MOST_DIRECT:
        return None
    return [mask for mask in order if mask < peers]


def swapped(x, mask, across=False):
    sections, peers = lax.axis_size("section"), lax.axis_size("mp")
    pairs = [
        (s * peers + i, ((s ^ 1) if across else s) * peers + (i ^ mask))
        for s in range(sections)
        for i in range(peers)
    ]
    return lax.ppermute(x, ("section", "mp"), pairs)


def from_peers(x, order=MIX_ORDER):
    masks = swap_masks(lax.axis_size("mp"), order)
    if masks is None:
        return [(None, lax.all_gather(x, "mp", axis=0, tiled=False))]
    return [(mask, swapped(x, mask)) for mask in masks]


def peer_blocks(masks, refs):
    peers = lax.axis_size("mp")
    me = lax.axis_index("mp")
    if masks == [None]:
        turned = [lax.rem(me + step, peers) for step in range(1, peers)]
        return [(peer, refs[0][peer]) for peer in turned]
    return [(me ^ mask, ref[...]) for mask, ref in zip(masks, refs)]


def rows_of(peer, count):
    return pl.ds(pl.multiple_of(peer * count, count), count)


def call(body, outs, *args, specs=None, scratch=(), limit=8):
    specs = specs or [pl.BlockSpec(memory_space=VMEM)] * len(args)
    return pl.pallas_call(
        body,
        in_specs=specs,
        out_specs=tuple(pl.BlockSpec(memory_space=VMEM) for _ in outs),
        out_shape=tuple(outs),
        scratch_shapes=list(scratch),
        compiler_params=pltpu.CompilerParams(vmem_limit_bytes=limit << 20),
    )(*args)


def add_part(peer, block, gain_ref, weight_ref, total_ref, squares):
    width = block.shape[1]
    rows = block.astype(F32)
    gain = gain_ref[:, rows_of(peer, width)].astype(F32)
    gained = (rows * gain).astype(BF16)
    for lane in range(0, width, LANES):
        tile = rows[:, lane : lane + LANES]
        squares = squares + tile * tile
    for kind in range(weight_ref.shape[0]):
        part = weight_ref[kind, rows_of(peer, width), :]
        total_ref[kind] += jnp.dot(gained, part, preferred_element_type=F32)
    return squares


def own_part(peer, block, gain_ref, weight_ref, total_ref, squares_ref):
    total_ref[...] = jnp.zeros_like(total_ref)
    squares = jnp.zeros(squares_ref.shape, F32)
    squares_ref[...] = add_part(peer, block, gain_ref, weight_ref, total_ref, squares)


def load_kernel(x_in, gain_in, qkv_in, out_in, table_ref, grid_in,
                x_ref, gain_ref, held_qkv, held_out, total_ref, squares_ref, bias_ref,
                grid_ref, sems):
    peers = lax.axis_size("mp")
    me = lax.axis_index("mp")
    width = x_in.shape[1]
    pairs = [(grid_in, grid_ref), (x_in, x_ref), (gain_in, gain_ref)]
    for step in range(peers):
        rows = rows_of(lax.rem(me + step, peers), width)
        pairs.append((qkv_in.at[:, rows, :], held_qkv.at[:, rows, :]))
    pairs.append((out_in, held_out))
    copies = [pltpu.make_async_copy(a, b, sems.at[i]) for i, (a, b) in enumerate(pairs)]
    for copy in copies:
        copy.start()
    heads, buckets = table_ref.shape
    length = grid_ref.shape[0]
    copies[0].wait()

    def one_head(head, carry):
        grid = grid_ref[...]
        bias = jnp.zeros(grid.shape, F32)
        for bucket in range(buckets):
            bias = jnp.where(grid == bucket, table_ref[head, bucket], bias)
        bias_ref[rows_of(head, length), :] = bias
        return carry

    lax.fori_loop(0, heads, one_head, 0)
    for copy in copies[1:4]:
        copy.wait()
    own_part(me, x_ref[...], gain_ref, held_qkv, total_ref, squares_ref)
    for copy in copies[4:]:
        copy.wait()


def own_kernel(x_ref, gain_ref, held_qkv, total_ref, squares_ref):
    own_part(lax.axis_index("mp"), x_ref[...], gain_ref, held_qkv, total_ref, squares_ref)


def add_kernel(masks, *refs):
    peer_refs = refs[: len(masks)]
    gain_ref, held_qkv, partial_ref, partial_squares, total_ref, squares_ref = refs[len(masks):]
    total_ref[...] = partial_ref[...]
    squares = partial_squares[...]
    for peer, block in peer_blocks(masks, peer_refs):
        squares = add_part(peer, block, gain_ref, held_qkv, total_ref, squares)
    squares_ref[...] = squares


def attend_kernel(masks, head_size, model_width, *refs):
    peer_refs = refs[: len(masks)]
    gain_ref, held_qkv, partial_ref, partial_squares, bias_ref, mix_ref, total_ref = refs[len(masks):]
    total_ref[...] = partial_ref[...]
    squares = partial_squares[...]
    for peer, block in peer_blocks(masks, peer_refs):
        squares = add_part(peer, block, gain_ref, held_qkv, total_ref, squares)
    mean_square = jnp.sum(squares, axis=1, keepdims=True) / model_width
    row_scale = lax.rsqrt(mean_square + NORM_EPSILON)
    length, local_qkv = mix_ref.shape
    score_scale = 1.0 / math.sqrt(head_size)
    block_heads = LANES // head_size
    lane = lax.broadcasted_iota(jnp.int32, (length, LANES), 1) // head_size
    for block in range(local_qkv // LANES):
        lanes = pl.ds(block * LANES, LANES)
        queries, keys, values = (total_ref[kind, :, lanes] * row_scale for kind in range(3))
        keys = keys.astype(BF16)
        values = values.astype(BF16)
        stacked = jnp.concatenate(
            [jnp.where(lane == head, queries, 0.0) for head in range(block_heads)], axis=0
        ).astype(BF16)
        scores = lax.dot_general(
            stacked, keys, (((1,), (1,)), ((), ())), preferred_element_type=F32)
        rows = pl.ds(block * block_heads * length, block_heads * length)
        scores = scores * score_scale + bias_ref[rows, :]
        weights = jnp.exp(scores - jnp.max(scores, axis=1, keepdims=True))
        probs = (weights / jnp.sum(weights, axis=1, keepdims=True)).astype(BF16)
        mixed = jnp.dot(probs, values, preferred_element_type=F32)
        mix = mixed[:length]
        for head in range(1, block_heads):
            mix = jnp.where(lane == head, mixed[head * length : (head + 1) * length], mix)
        mix_ref[:, lanes] = mix.astype(BF16)


def out_part_kernel(masks, *refs):
    peer_refs = refs[: len(masks)]
    own_ref, held_out, stream_ref, total_ref = refs[len(masks):]
    total_ref[...] = add_mixes(stream_ref[...].astype(F32), [(lax.axis_index("mp"), own_ref[...])]
                               + peer_blocks(masks, peer_refs), held_out)


def add_mixes(total, blocks, held_out):
    for peer, block in blocks:
        part = held_out[rows_of(peer, block.shape[1]), :]
        total += jnp.dot(block, part, preferred_element_type=F32)
    return total


def out_kernel(masks, keep_section, *refs):
    peer_refs = refs[: len(masks)]
    held_out, partial_ref, kept_ref, result_ref = refs[len(masks):]
    total = add_mixes(partial_ref[...], peer_blocks(masks, peer_refs), held_out)
    result = total.astype(BF16)
    if keep_section is not None:
        result = jnp.where(lax.axis_index("section") == keep_section, kept_ref[...], result)
    result_ref[...] = result


def pick_kernel(section, a_ref, b_ref, o_ref):
    o_ref[...] = jnp.where(lax.axis_index("section") == section, a_ref[...], b_ref[...])


def pick(section, a, b):
    return call(lambda *refs: pick_kernel(section, *refs), [VMEM(a.shape, a.dtype)], a, b)[0]


def shards(micro_inputs, qkv_weight, out_weight, norm_gain, position_bias):
    sections = lax.axis_size("section")
    peers = lax.axis_size("mp")
    length = micro_inputs.shape[1]
    model_width = qkv_weight.shape[1]
    local_heads, bucket_count = position_bias.shape
    local_qkv = qkv_weight.shape[3]
    head_size = local_qkv // local_heads
    weights_qkv = jnp.transpose(qkv_weight[0], (1, 0, 2))
    weights_out = out_weight[0]
    bucket_grid = jnp.asarray(bucket_table(length, bucket_count, REACH))

    total = VMEM((3, length, local_qkv), F32)
    squares = VMEM((length, LANES), F32)
    raw = micro_inputs[0]

    def stay(x):
        return pltpu.with_memory_space_constraint(x, pltpu.HBM)

    def load():
        vm = pl.BlockSpec(memory_space=VMEM)
        hbm = pl.BlockSpec(memory_space=pltpu.HBM)
        sm = pl.BlockSpec(memory_space=pltpu.SMEM)
        return call(
            load_kernel,
            [
                VMEM(raw.shape, BF16), VMEM(norm_gain.shape, BF16),
                VMEM(weights_qkv.shape, BF16), VMEM(weights_out.shape, BF16),
                total, squares, VMEM((local_heads * length, length), F32),
            ],
            stay(raw), stay(norm_gain), stay(weights_qkv), stay(weights_out),
            position_bias, stay(bucket_grid),
            specs=[hbm, hbm, hbm, hbm, sm, hbm],
            scratch=[VMEM((length, length), jnp.int32), pltpu.SemaphoreType.DMA((peers + 4,))],
        )

    def add_own(section_in):
        return call(own_kernel, [total, squares], section_in, gain, held_qkv)

    def attend(others, parts):
        for early in others[:-1]:
            masks = [early[0]]
            parts = call(
                lambda *refs: add_kernel(masks, *refs), [total, squares],
                early[1], gain, held_qkv, *parts)
        late = others[-1:]
        masks = [mask for mask, block in late]
        return call(
            lambda *refs: attend_kernel(masks, head_size, model_width, *refs),
            [VMEM((length, local_qkv), BF16)],
            *[block for mask, block in late], gain, held_qkv, *parts, bias,
            scratch=[total],
        )[0]

    def project(mixes, mix, stream, keep_section=None, kept=None):
        early, late = mixes[:-2], mixes[-2:]
        early_masks = [mask for mask, block in early]
        late_masks = [mask for mask, block in late]
        partial = call(
            lambda *refs: out_part_kernel(early_masks, *refs),
            [VMEM(stream.shape, F32)],
            *[block for mask, block in early], mix, held_out, stream,
        )[0]
        return call(
            lambda *refs: out_kernel(late_masks, keep_section, *refs),
            [VMEM(stream.shape, BF16)],
            *[block for mask, block in late], held_out, partial, stream if kept is None else kept,
        )[0]

    def layer(section_in, others, parts=None, keep_section=None, kept=None):
        mix = attend(others, parts or add_own(section_in))
        return project(from_peers(mix), mix, section_in, keep_section, kept)

    def handed_on(out):
        section_in = swapped(out, 0, across=True)
        early = [mask for mask in ACROSS if mask < peers]
        others = [(mask, swapped(out, mask, across=True)) for mask in early]
        others += [(mask, swapped(section_in, mask)) for mask in swap_masks(peers, REST_ORDER) if mask not in early]
        return section_in, others

    def rotated(x, by):
        return lax.ppermute(x, "section", [(i, (i + by) % sections) for i in range(sections)])

    others = from_peers(raw, FIRST_ORDER)
    current, gain, held_qkv, held_out, *parts, bias = load()
    if sections == 2 and swap_masks(peers):
        current, others = handed_on(layer(current, others, parts, 1, current))
        current, others = handed_on(layer(current, others))
        return layer(current, others, None, 0, current)[None]
    ticks = 2 * sections - 1
    result = current
    for tick in range(ticks):
        if tick + 1 < sections:
            raw = rotated(raw, -1)
        out = layer(current, others, parts)
        parts = None
        done = tick - (sections - 1)
        if tick + 1 < ticks:
            sent = rotated(out, 1)
            current = pick(0, raw, sent)
            others = from_peers(current)
        if done >= 0:
            owned = rotated(out, done + 1) if done + 1 < sections else out
            result = pick(done, owned, result)
    return result[None]


def solution(mesh):
    in_specs = (
        P(("dp", "section"), None, "mp"),
        P("section", None, None, "mp"),
        P("section", None, "mp"),
        P("section", None),
        P("mp", None),
    )
    out_specs = P(("dp", "section"), None, "mp")
    return jax.shard_map(shards, mesh=mesh, in_specs=in_specs, out_specs=out_specs, check_vma=False)
```

```python
import math

import jax
import jax.numpy as jnp
import numpy as np
from jax import lax
from jax.experimental import pallas as pl
from jax.experimental.pallas import tpu as pltpu
from jax.sharding import PartitionSpec as P


REACH = 128
NORM_EPSILON = 0.1
MOST_DIRECT = 4
FIRST_ORDER = (3, 1, 2)
MIX_ORDER = (2, 3, 1)
REST_ORDER = (3, 1)
FAR = 2
LANES = 128
F32 = jnp.float32
BF16 = jnp.bfloat16
VMEM = pltpu.VMEM


def bucket_table(length, bucket_count, reach_limit):
    offset = np.arange(length)[None, :] - np.arange(length)[:, None]
    half_count = bucket_count // 2
    upper_side = (offset > 0).astype(np.int32) * half_count
    distance = np.abs(offset)
    exact_count = half_count // 2
    scaled = (
        np.log(np.maximum(distance, 1) / exact_count)
        / np.log(reach_limit / exact_count)
        * (half_count - exact_count)
    )
    far_bucket = np.minimum(exact_count + scaled.astype(np.int32), half_count - 1)
    return (upper_side + np.where(distance < exact_count, distance, far_bucket)).astype(np.int32)


def swap_masks(peers, order=MIX_ORDER):
    if peers & (peers - 1) or peers > MOST_DIRECT:
        return None
    return [mask for mask in order if mask < peers]


def permuted(x, target):
    sections, peers = lax.axis_size("section"), lax.axis_size("mp")
    pairs = []
    for s in range(sections):
        for i in range(peers):
            to_section, to_place = target(s, i)
            pairs.append((s * peers + i, to_section * peers + to_place))
    return lax.ppermute(x, ("section", "mp"), pairs)


def swapped(x, mask, section=None):
    return permuted(x, lambda s, i: (s, i ^ (mask if section in (None, s) else 1)))


def crossed(x, mask, section):
    return permuted(x, lambda s, i: (s ^ 1, i ^ mask if s == section else i))


def from_peers(x, order=MIX_ORDER, section=None):
    masks = swap_masks(lax.axis_size("mp"), order)
    if masks is None:
        return [(None, (lax.all_gather(x, "mp", axis=0, tiled=False),))]
    return [(mask, (swapped(x, mask, section),)) for mask in masks]


def chosen(refs):
    if len(refs) == 1:
        return refs[0][...]
    return jnp.where(lax.axis_index("section") == 0, refs[0][...], refs[1][...])


def peer_blocks(masks, groups):
    peers = lax.axis_size("mp")
    me = lax.axis_index("mp")
    if masks == [None]:
        turned = [lax.rem(me + step, peers) for step in range(1, peers)]
        return [(peer, groups[0][0][peer]) for peer in turned]
    return [(me ^ mask, chosen(refs)) for mask, refs in zip(masks, groups)]


def grouped(refs, sizes):
    groups = []
    for size in sizes:
        groups.append(refs[:size])
        refs = refs[size:]
    return groups, refs


def rows_of(peer, count):
    return pl.ds(pl.multiple_of(peer * count, count), count)


def call(body, outs, *args, specs=None, scratch=(), limit=8):
    specs = specs or [pl.BlockSpec(memory_space=VMEM)] * len(args)
    run = pl.pallas_call(
        body,
        in_specs=specs,
        out_specs=tuple(pl.BlockSpec(memory_space=VMEM) for _ in outs),
        out_shape=tuple(outs),
        scratch_shapes=list(scratch),
        compiler_params=pltpu.CompilerParams(vmem_limit_bytes=limit << 20),
    )
    return run(*args)


def add_part(peer, block, gain_ref, weight_ref, total_ref, squares):
    width = block.shape[1]
    rows = block.astype(F32)
    gain = gain_ref[:, rows_of(peer, width)].astype(F32)
    gained = (rows * gain).astype(BF16)
    for lane in range(0, width, LANES):
        tile = rows[:, lane : lane + LANES]
        squares = squares + tile * tile
    for kind in range(weight_ref.shape[0]):
        part = weight_ref[kind, rows_of(peer, width), :]
        total_ref[kind] += jnp.dot(gained, part, preferred_element_type=F32)
    return squares


def own_part(peer, block, gain_ref, weight_ref, total_ref, squares_ref):
    total_ref[...] = jnp.zeros_like(total_ref)
    squares = jnp.zeros(squares_ref.shape, F32)
    squares_ref[...] = add_part(peer, block, gain_ref, weight_ref, total_ref, squares)


def load_kernel(x_in, gain_in, qkv_in, table_ref, grid_in,
                x_ref, gain_ref, held_qkv, total_ref, squares_ref, bias_ref,
                grid_ref, sems):
    peers = lax.axis_size("mp")
    me = lax.axis_index("mp")
    width = x_in.shape[1]
    pairs = [(grid_in, grid_ref), (x_in, x_ref), (gain_in, gain_ref)]
    for step in range(peers):
        rows = rows_of(lax.rem(me + step, peers), width)
        pairs.append((qkv_in.at[:, rows, :], held_qkv.at[:, rows, :]))
    copies = [pltpu.make_async_copy(a, b, sems.at[i]) for i, (a, b) in enumerate(pairs)]
    for copy in copies:
        copy.start()
    heads, buckets = table_ref.shape
    length = grid_ref.shape[0]
    copies[0].wait()

    def one_head(head, carry):
        grid = grid_ref[...]
        bias = jnp.zeros(grid.shape, F32)
        for bucket in range(buckets):
            bias = jnp.where(grid == bucket, table_ref[head, bucket], bias)
        bias_ref[rows_of(head, length), :] = bias
        return carry

    lax.fori_loop(0, heads, one_head, 0)
    for copy in copies[1:4]:
        copy.wait()
    own_part(me, x_ref[...], gain_ref, held_qkv, total_ref, squares_ref)
    for copy in copies[4:]:
        copy.wait()


def fetch_kernel(whole_in, held_ref, sems):
    count = sems.shape[0]
    rows = whole_in.shape[0] // count
    copies = [
        pltpu.make_async_copy(
            whole_in.at[pl.ds(part * rows, rows), :],
            held_ref.at[pl.ds(part * rows, rows), :],
            sems.at[part],
        )
        for part in range(count)
    ]
    for copy in copies:
        copy.start()
    for copy in copies:
        copy.wait()


def own_kernel(*refs):
    *block_refs, gain_ref, held_qkv, stream_ref, total_ref, squares_ref = refs
    block = chosen(block_refs)
    stream_ref[...] = block
    own_part(lax.axis_index("mp"), block, gain_ref, held_qkv, total_ref, squares_ref)


def add_kernel(masks, sizes, *refs):
    peer_refs, rest = grouped(refs, sizes)
    gain_ref, held_qkv, partial_ref, partial_squares, total_ref, squares_ref = rest
    total_ref[...] = partial_ref[...]
    squares = partial_squares[...]
    for peer, block in peer_blocks(masks, peer_refs):
        squares = add_part(peer, block, gain_ref, held_qkv, total_ref, squares)
    squares_ref[...] = squares


def attend_kernel(masks, sizes, head_size, model_width, *refs):
    peer_refs, rest = grouped(refs, sizes)
    gain_ref, held_qkv, partial_ref, partial_squares, bias_ref, mix_ref, total_ref = rest
    total_ref[...] = partial_ref[...]
    squares = partial_squares[...]
    for peer, block in peer_blocks(masks, peer_refs):
        squares = add_part(peer, block, gain_ref, held_qkv, total_ref, squares)
    mean_square = jnp.sum(squares, axis=1, keepdims=True) / model_width
    row_scale = lax.rsqrt(mean_square + NORM_EPSILON)
    length, local_qkv = mix_ref.shape
    score_scale = 1.0 / math.sqrt(head_size)
    block_heads = LANES // head_size
    lane = lax.broadcasted_iota(jnp.int32, (length, LANES), 1) // head_size
    for block in range(local_qkv // LANES):
        lanes = pl.ds(block * LANES, LANES)
        queries, keys, values = (total_ref[kind, :, lanes] * row_scale for kind in range(3))
        keys = keys.astype(BF16)
        values = values.astype(BF16)
        stacked = jnp.concatenate(
            [jnp.where(lane == head, queries, 0.0) for head in range(block_heads)], axis=0
        ).astype(BF16)
        scores = lax.dot_general(
            stacked, keys, (((1,), (1,)), ((), ())), preferred_element_type=F32)
        rows = pl.ds(block * block_heads * length, block_heads * length)
        scores = scores * score_scale + bias_ref[rows, :]
        weights = jnp.exp(scores - jnp.max(scores, axis=1, keepdims=True))
        probs = (weights / jnp.sum(weights, axis=1, keepdims=True)).astype(BF16)
        mixed = jnp.dot(probs, values, preferred_element_type=F32)
        mix = mixed[:length]
        for head in range(1, block_heads):
            mix = jnp.where(lane == head, mixed[head * length : (head + 1) * length], mix)
        mix_ref[:, lanes] = mix.astype(BF16)


def out_part_kernel(masks, *refs):
    peer_refs, rest = grouped(refs, [1] * len(masks))
    own_ref, held_out, stream_ref, total_ref = rest
    total_ref[...] = add_mixes(stream_ref[...].astype(F32), [(lax.axis_index("mp"), own_ref[...])]
                               + peer_blocks(masks, peer_refs), held_out)


def add_mixes(total, blocks, held_out):
    for peer, block in blocks:
        part = held_out[rows_of(peer, block.shape[1]), :]
        total += jnp.dot(block, part, preferred_element_type=F32)
    return total


def out_kernel(masks, keep_section, *refs):
    peer_refs, rest = grouped(refs, [1] * len(masks))
    held_out, partial_ref, kept_ref, result_ref = rest
    total = add_mixes(partial_ref[...], peer_blocks(masks, peer_refs), held_out)
    result = total.astype(BF16)
    if keep_section is not None:
        result = jnp.where(lax.axis_index("section") == keep_section, kept_ref[...], result)
    result_ref[...] = result


def send_kernel(masks, *refs):
    peer_refs, rest = grouped(refs, [1] * len(masks))
    held_out, partial_ref, own_ref, far_ref, to_own_ref, to_far_ref = rest
    total = add_mixes(partial_ref[...], peer_blocks(masks, peer_refs), held_out)
    result = total.astype(BF16)
    last = lax.axis_index("section") == lax.axis_size("section") - 1
    to_own_ref[...] = jnp.where(last, own_ref[...], result)
    to_far_ref[...] = jnp.where(last, far_ref[...], result)


def pick_kernel(section, a_ref, b_ref, o_ref):
    o_ref[...] = jnp.where(lax.axis_index("section") == section, a_ref[...], b_ref[...])


def pick(section, a, b):
    return call(lambda *refs: pick_kernel(section, *refs), [VMEM(a.shape, a.dtype)], a, b)[0]


def shards(micro_inputs, qkv_weight, out_weight, norm_gain, position_bias):
    sections = lax.axis_size("section")
    peers = lax.axis_size("mp")
    length = micro_inputs.shape[1]
    model_width = qkv_weight.shape[1]
    local_heads, bucket_count = position_bias.shape
    local_qkv = qkv_weight.shape[3]
    head_size = local_qkv // local_heads
    weights_qkv = jnp.transpose(qkv_weight[0], (1, 0, 2))
    weights_out = out_weight[0]
    bucket_grid = jnp.asarray(bucket_table(length, bucket_count, REACH))

    total = VMEM((3, length, local_qkv), F32)
    squares = VMEM((length, LANES), F32)
    raw = micro_inputs[0]

    def stay(x):
        return pltpu.with_memory_space_constraint(x, pltpu.HBM)

    def load():
        vm = pl.BlockSpec(memory_space=VMEM)
        hbm = pl.BlockSpec(memory_space=pltpu.HBM)
        sm = pl.BlockSpec(memory_space=pltpu.SMEM)
        return call(
            load_kernel,
            [
                VMEM(raw.shape, BF16), VMEM(norm_gain.shape, BF16),
                VMEM(weights_qkv.shape, BF16),
                total, squares, VMEM((local_heads * length, length), F32),
            ],
            stay(raw), stay(norm_gain), stay(weights_qkv),
            position_bias, stay(bucket_grid),
            specs=[hbm, hbm, hbm, sm, hbm],
            scratch=[VMEM((length, length), jnp.int32), pltpu.SemaphoreType.DMA((peers + 3,))],
        )

    def fetch(x):
        return call(
            fetch_kernel, [VMEM(x.shape, x.dtype)], stay(x),
            specs=[pl.BlockSpec(memory_space=pltpu.HBM)],
            scratch=[pltpu.SemaphoreType.DMA((peers,))],
        )[0]

    def add_own(blocks):
        stream, *parts = call(
            own_kernel, [VMEM(raw.shape, BF16), total, squares], *blocks, gain, held_qkv)
        return stream, parts

    def attend(others, parts):
        for mask, blocks in others[:-1]:
            parts = call(
                lambda *refs, m=mask, n=len(blocks): add_kernel([m], [n], *refs),
                [total, squares], *blocks, gain, held_qkv, *parts)
        late = others[-1:]
        masks = [mask for mask, blocks in late]
        sizes = [len(blocks) for mask, blocks in late]
        return call(
            lambda *refs: attend_kernel(masks, sizes, head_size, model_width, *refs),
            [VMEM((length, local_qkv), BF16)],
            *[x for mask, blocks in late for x in blocks], gain, held_qkv, *parts, bias,
            scratch=[total],
        )[0]

    def project(mixes, mix, stream, keep_section=None, kept=None):
        early, late = mixes[:-2], mixes[-2:]
        early_masks = [mask for mask, blocks in early]
        late_masks = [mask for mask, blocks in late]
        partial = call(
            lambda *refs: out_part_kernel(early_masks, *refs),
            [VMEM(stream.shape, F32)],
            *[blocks[0] for mask, blocks in early], mix, held_out, stream,
        )[0]
        if isinstance(kept, tuple):
            return call(
                lambda *refs: send_kernel(late_masks, *refs),
                [VMEM(stream.shape, BF16)] * 2,
                *[blocks[0] for mask, blocks in late], held_out, partial, *kept,
            )
        return call(
            lambda *refs: out_kernel(late_masks, keep_section, *refs),
            [VMEM(stream.shape, BF16)],
            *[blocks[0] for mask, blocks in late], held_out, partial, stream if kept is None else kept,
        )[0]

    def layer(stream, others, parts, keep_section=None, kept=None, section=None):
        mix = attend(others, parts)
        mixes = from_peers(mix, section=section)
        return project(mixes, mix, stream, keep_section, kept)

    def handed_on(out, far):
        own = crossed(out, 0, 0)
        others = [(FAR, (crossed(far, FAR, 0),))]
        others += [(mask, (swapped(own, mask, 1),)) for mask in REST_ORDER]
        return own, others

    def rotated(x, by):
        return lax.ppermute(x, "section", [(i, (i + by) % sections) for i in range(sections)])

    if sections == 2 and peers == MOST_DIRECT:
        others = [
            (mask, (swapped(raw, mask, 0 if mask in (3,) else None),))
            for mask in FIRST_ORDER
        ]
        ahead = crossed(raw, 3, 1)
        stream, gain, held_qkv, *parts, bias = load()
        held_out = fetch(weights_out)
        far = dict(others)[FAR][0]
        out, far = layer(stream, others, parts, None, (stream, far))
        stream, others = handed_on(out, far)
        others = [(mask, (ahead, *blocks) if mask == 3 else blocks) for mask, blocks in others]
        stream, parts = add_own((stream,))
        out = layer(stream, others, parts)
        finished, others = handed_on(out, out)
        stream, parts = add_own((finished,))
        return layer(stream, others, parts, 0, finished)[None]
    others = from_peers(raw, FIRST_ORDER)
    current, gain, held_qkv, *parts, bias = load()
    held_out = fetch(weights_out)
    ticks = 2 * sections - 1
    result = current
    for tick in range(ticks):
        if tick + 1 < sections:
            raw = rotated(raw, -1)
        out = layer(current, others, parts)
        done = tick - (sections - 1)
        if tick + 1 < ticks:
            sent = rotated(out, 1)
            current = pick(0, raw, sent)
            others = from_peers(current)
            current, parts = add_own((current,))
        if done >= 0:
            owned = rotated(out, done + 1) if done + 1 < sections else out
            result = pick(done, owned, result)
    return result[None]


def solution(mesh):
    in_specs = (
        P(("dp", "section"), None, "mp"),
        P("section", None, None, "mp"),
        P("section", None, "mp"),
        P("section", None),
        P("mp", None),
    )
    out_specs = P(("dp", "section"), None, "mp")
    return jax.shard_map(shards, mesh=mesh, in_specs=in_specs, out_specs=out_specs, check_vma=False)
```

```python
import math

import jax
import jax.numpy as jnp
import numpy as np
from jax import lax
from jax.experimental import pallas as pl
from jax.experimental.pallas import tpu as pltpu
from jax.sharding import PartitionSpec as P


REACH = 128
NORM_EPSILON = 0.1
MOST_DIRECT = 4
FIRST_ORDER = (3, 1, 2)
MIX_ORDER = (2, 1, 3)
REST_ORDER = (3, 1)
FAR = 2
LANES = 128
DIRECT = 2
F32 = jnp.float32
BF16 = jnp.bfloat16
VMEM = pltpu.VMEM


def bucket_table(length, bucket_count, reach_limit):
    offset = np.arange(length)[None, :] - np.arange(length)[:, None]
    half_count = bucket_count // 2
    upper_side = (offset > 0).astype(np.int32) * half_count
    distance = np.abs(offset)
    exact_count = half_count // 2
    scaled = (
        np.log(np.maximum(distance, 1) / exact_count)
        / np.log(reach_limit / exact_count)
        * (half_count - exact_count)
    )
    far_bucket = np.minimum(exact_count + scaled.astype(np.int32), half_count - 1)
    return (upper_side + np.where(distance < exact_count, distance, far_bucket)).astype(np.int32)


def swap_masks(peers, order=MIX_ORDER):
    if peers & (peers - 1) or peers > MOST_DIRECT:
        return None
    return [mask for mask in order if mask < peers]


def permuted(x, target):
    sections, peers = lax.axis_size("section"), lax.axis_size("mp")
    pairs = []
    for s in range(sections):
        for i in range(peers):
            to_section, to_place = target(s, i)
            pairs.append((s * peers + i, to_section * peers + to_place))
    return lax.ppermute(x, ("section", "mp"), pairs)


def swapped(x, mask, section=None):
    return permuted(x, lambda s, i: (s, i ^ (mask if section in (None, s) else 1)))


def crossed(x, mask, section):
    return permuted(x, lambda s, i: (s ^ 1, i ^ mask if s == section else i))


def from_peers(x, order=MIX_ORDER, section=None):
    masks = swap_masks(lax.axis_size("mp"), order)
    if masks is None:
        return [(None, (lax.all_gather(x, "mp", axis=0, tiled=False),))]
    return [(mask, (swapped(x, mask, section),)) for mask in masks]


def chosen(refs):
    if len(refs) == 1:
        return refs[0][...]
    return jnp.where(lax.axis_index("section") == 0, refs[0][...], refs[1][...])


def peer_blocks(masks, groups):
    peers = lax.axis_size("mp")
    me = lax.axis_index("mp")
    if masks == [None]:
        turned = [lax.rem(me + step, peers) for step in range(1, peers)]
        return [(peer, groups[0][0][peer]) for peer in turned]
    return [(me ^ mask, chosen(refs)) for mask, refs in zip(masks, groups)]


def grouped(refs, sizes):
    groups = []
    for size in sizes:
        groups.append(refs[:size])
        refs = refs[size:]
    return groups, refs


def rows_of(peer, count):
    return pl.ds(pl.multiple_of(peer * count, count), count)


def call(body, outs, *args, specs=None, outs_specs=None, scratch=(), limit=8):
    specs = specs or [pl.BlockSpec(memory_space=VMEM)] * len(args)
    run = pl.pallas_call(
        body,
        in_specs=specs,
        out_specs=tuple(outs_specs or [pl.BlockSpec(memory_space=VMEM) for _ in outs]),
        out_shape=tuple(outs),
        scratch_shapes=list(scratch),
        compiler_params=pltpu.CompilerParams(vmem_limit_bytes=limit << 20),
    )
    return run(*args)


def add_part(peer, block, gain_ref, weight_ref, total_ref, squares):
    width = block.shape[1]
    rows = block.astype(F32)
    gain = gain_ref[:, rows_of(peer, width)].astype(F32)
    gained = (rows * gain).astype(BF16)
    for lane in range(0, width, LANES):
        tile = rows[:, lane : lane + LANES]
        squares = squares + tile * tile
    for kind in range(weight_ref.shape[0]):
        part = weight_ref[kind, rows_of(peer, width), :]
        total_ref[kind] += jnp.dot(gained, part, preferred_element_type=F32)
    return squares


def own_part(peer, block, gain_ref, weight_ref, total_ref, squares_ref):
    total_ref[...] = jnp.zeros_like(total_ref)
    squares = jnp.zeros(squares_ref.shape, F32)
    squares_ref[...] = add_part(peer, block, gain_ref, weight_ref, total_ref, squares)


def load_kernel(x_in, gain_in, qkv_in, table_ref, grid_in,
                x_ref, gain_ref, held_qkv, total_ref, squares_ref, bias_ref,
                grid_ref, sems):
    peers = lax.axis_size("mp")
    me = lax.axis_index("mp")
    width = x_in.shape[1]
    pairs = [(grid_in, grid_ref), (x_in, x_ref), (gain_in, gain_ref)]
    for step in range(peers):
        rows = rows_of(lax.rem(me + step, peers), width)
        pairs.append((qkv_in.at[:, rows, :], held_qkv.at[:, rows, :]))
    copies = [pltpu.make_async_copy(a, b, sems.at[i]) for i, (a, b) in enumerate(pairs)]
    for copy in copies:
        copy.start()
    heads, buckets = table_ref.shape
    length = grid_ref.shape[0]
    copies[0].wait()

    def one_head(head, carry):
        grid = grid_ref[...]
        bias = jnp.zeros(grid.shape, F32)
        for bucket in range(buckets):
            bias = jnp.where(grid == bucket, table_ref[head, bucket], bias)
        bias_ref[rows_of(head, length), :] = bias
        return carry

    lax.fori_loop(0, heads, one_head, 0)
    for copy in copies[1:4]:
        copy.wait()
    own_part(me, x_ref[...], gain_ref, held_qkv, total_ref, squares_ref)
    for copy in copies[4:]:
        copy.wait()


def fetch_kernel(whole_in, held_ref, sems):
    count = sems.shape[0]
    rows = whole_in.shape[0] // count
    copies = [
        pltpu.make_async_copy(
            whole_in.at[pl.ds(part * rows, rows), :],
            held_ref.at[pl.ds(part * rows, rows), :],
            sems.at[part],
        )
        for part in range(count)
    ]
    for copy in copies:
        copy.start()
    for copy in copies:
        copy.wait()


def own_kernel(*refs):
    *block_refs, gain_ref, held_qkv, stream_ref, total_ref, squares_ref = refs
    block = chosen(block_refs)
    stream_ref[...] = block
    own_part(lax.axis_index("mp"), block, gain_ref, held_qkv, total_ref, squares_ref)


def add_kernel(masks, sizes, *refs):
    peer_refs, rest = grouped(refs, sizes)
    gain_ref, held_qkv, partial_ref, partial_squares, total_ref, squares_ref = rest
    total_ref[...] = partial_ref[...]
    squares = partial_squares[...]
    for peer, block in peer_blocks(masks, peer_refs):
        squares = add_part(peer, block, gain_ref, held_qkv, total_ref, squares)
    squares_ref[...] = squares


def attend_kernel(masks, sizes, head_size, model_width, *refs):
    peer_refs, rest = grouped(refs, sizes)
    gain_ref, held_qkv, partial_ref, partial_squares, bias_ref, mix_ref, total_ref = rest
    total_ref[...] = partial_ref[...]
    squares = partial_squares[...]
    for peer, block in peer_blocks(masks, peer_refs):
        squares = add_part(peer, block, gain_ref, held_qkv, total_ref, squares)
    mean_square = jnp.sum(squares, axis=1, keepdims=True) / model_width
    row_scale = lax.rsqrt(mean_square + NORM_EPSILON)
    length, local_qkv = mix_ref.shape
    score_scale = 1.0 / math.sqrt(head_size)
    block_heads = LANES // head_size
    lane = lax.broadcasted_iota(jnp.int32, (length, LANES), 1) // head_size
    for block in range(local_qkv // LANES):
        lanes = pl.ds(block * LANES, LANES)
        queries, keys, values = (total_ref[kind, :, lanes] * row_scale for kind in range(3))
        keys = keys.astype(BF16)
        values = values.astype(BF16)
        stacked = jnp.concatenate(
            [jnp.where(lane == head, queries, 0.0) for head in range(block_heads)], axis=0
        ).astype(BF16)
        scores = lax.dot_general(
            stacked, keys, (((1,), (1,)), ((), ())), preferred_element_type=F32)
        rows = pl.ds(block * block_heads * length, block_heads * length)
        scores = scores * score_scale + bias_ref[rows, :]
        weights = jnp.exp(scores - jnp.max(scores, axis=1, keepdims=True))
        probs = (weights / jnp.sum(weights, axis=1, keepdims=True)).astype(BF16)
        mixed = jnp.dot(probs, values, preferred_element_type=F32)
        mix = mixed[:length]
        for head in range(1, block_heads):
            mix = jnp.where(lane == head, mixed[head * length : (head + 1) * length], mix)
        mix_ref[:, lanes] = mix.astype(BF16)


def out_part_kernel(masks, *refs):
    peer_refs, rest = grouped(refs, [1] * len(masks))
    own_ref, held_out, stream_ref, total_ref = rest
    total_ref[...] = add_mixes(stream_ref[...].astype(F32), [(lax.axis_index("mp"), own_ref[...])]
                               + peer_blocks(masks, peer_refs), held_out)


def add_mixes(total, blocks, held_out):
    for peer, block in blocks:
        part = held_out[rows_of(peer, block.shape[1]), :]
        total += jnp.dot(block, part, preferred_element_type=F32)
    return total


def out_kernel(masks, keep_section, *refs):
    peer_refs, rest = grouped(refs, [1] * len(masks))
    held_out, partial_ref, kept_ref, result_ref = rest
    total = add_mixes(partial_ref[...], peer_blocks(masks, peer_refs), held_out)
    result = total.astype(BF16)
    if keep_section is not None:
        result = jnp.where(lax.axis_index("section") == keep_section, kept_ref[...], result)
    result_ref[...] = result


def last_kernel(masks, keep_section, *refs):
    peer_refs, rest = grouped(refs, [1] * len(masks))
    held_out, partial_ref, kept_ref, result_out, result_ref, sems = rest
    blocks = peer_blocks(masks, peer_refs)
    half = result_ref.shape[2]
    copies = []
    for part in range(result_ref.shape[0]):
        lanes = pl.ds(part * half, half)
        total = partial_ref[:, lanes]
        for peer, block in blocks:
            weights = held_out[rows_of(peer, block.shape[1]), lanes]
            total += jnp.dot(block, weights, preferred_element_type=F32)
        result = jnp.where(
            lax.axis_index("section") == keep_section, kept_ref[:, lanes], total.astype(BF16))
        result_ref[part] = result
        copy = pltpu.make_async_copy(result_ref.at[part], result_out.at[:, lanes], sems.at[part])
        copy.start()
        copies.append(copy)
    for copy in copies:
        copy.wait()


def send_kernel(masks, *refs):
    peer_refs, rest = grouped(refs, [1] * len(masks))
    held_out, partial_ref, own_ref, far_ref, to_own_ref, to_far_ref = rest
    total = add_mixes(partial_ref[...], peer_blocks(masks, peer_refs), held_out)
    result = total.astype(BF16)
    last = lax.axis_index("section") == lax.axis_size("section") - 1
    to_own_ref[...] = jnp.where(last, own_ref[...], result)
    to_far_ref[...] = jnp.where(last, far_ref[...], result)


def pick_kernel(section, a_ref, b_ref, o_ref):
    o_ref[...] = jnp.where(lax.axis_index("section") == section, a_ref[...], b_ref[...])


def pick(section, a, b):
    return call(lambda *refs: pick_kernel(section, *refs), [VMEM(a.shape, a.dtype)], a, b)[0]


def shards(micro_inputs, qkv_weight, out_weight, norm_gain, position_bias):
    sections = lax.axis_size("section")
    peers = lax.axis_size("mp")
    length = micro_inputs.shape[1]
    model_width = qkv_weight.shape[1]
    local_heads, bucket_count = position_bias.shape
    local_qkv = qkv_weight.shape[3]
    head_size = local_qkv // local_heads
    weights_qkv = jnp.transpose(qkv_weight[0], (1, 0, 2))
    weights_out = out_weight[0]
    bucket_grid = jnp.asarray(bucket_table(length, bucket_count, REACH))

    total = VMEM((3, length, local_qkv), F32)
    squares = VMEM((length, LANES), F32)
    raw = micro_inputs[0]

    def stay(x):
        return pltpu.with_memory_space_constraint(x, pltpu.HBM)

    def load():
        vm = pl.BlockSpec(memory_space=VMEM)
        hbm = pl.BlockSpec(memory_space=pltpu.HBM)
        sm = pl.BlockSpec(memory_space=pltpu.SMEM)
        return call(
            load_kernel,
            [
                VMEM(raw.shape, BF16), VMEM(norm_gain.shape, BF16),
                VMEM(weights_qkv.shape, BF16),
                total, squares, VMEM((local_heads * length, length), F32),
            ],
            stay(raw), stay(norm_gain), stay(weights_qkv),
            position_bias, stay(bucket_grid),
            specs=[hbm, hbm, hbm, sm, hbm],
            scratch=[VMEM((length, length), jnp.int32), pltpu.SemaphoreType.DMA((peers + 3,))],
        )

    def fetch(x):
        return call(
            fetch_kernel, [VMEM(x.shape, x.dtype)], stay(x),
            specs=[pl.BlockSpec(memory_space=pltpu.HBM)],
            scratch=[pltpu.SemaphoreType.DMA((peers,))],
        )[0]

    def add_own(blocks):
        stream, *parts = call(
            own_kernel, [VMEM(raw.shape, BF16), total, squares], *blocks, gain, held_qkv)
        return stream, parts

    def attend(others, parts):
        for mask, blocks in others[:-1]:
            parts = call(
                lambda *refs, m=mask, n=len(blocks): add_kernel([m], [n], *refs),
                [total, squares], *blocks, gain, held_qkv, *parts)
        late = others[-1:]
        masks = [mask for mask, blocks in late]
        sizes = [len(blocks) for mask, blocks in late]
        return call(
            lambda *refs: attend_kernel(masks, sizes, head_size, model_width, *refs),
            [VMEM((length, local_qkv), BF16)],
            *[x for mask, blocks in late for x in blocks], gain, held_qkv, *parts, bias,
            scratch=[total],
        )[0]

    def project(mixes, mix, stream, keep_section=None, kept=None):
        early, late = mixes[:-2], mixes[-2:]
        early_masks = [mask for mask, blocks in early]
        late_masks = [mask for mask, blocks in late]
        partial = call(
            lambda *refs: out_part_kernel(early_masks, *refs),
            [VMEM(stream.shape, F32)],
            *[blocks[0] for mask, blocks in early], mix, held_out, stream,
        )[0]
        if keep_section == 0:
            halves = VMEM((DIRECT, length, stream.shape[1] // DIRECT), BF16)
            return call(
                lambda *refs: last_kernel(late_masks, keep_section, *refs),
                [jax.ShapeDtypeStruct(stream.shape, BF16)],
                *[blocks[0] for mask, blocks in late], held_out, partial, kept,
                outs_specs=[pl.BlockSpec(memory_space=pltpu.HBM)],
                scratch=[halves, pltpu.SemaphoreType.DMA((DIRECT,))],
            )[0]
        if isinstance(kept, tuple):
            return call(
                lambda *refs: send_kernel(late_masks, *refs),
                [VMEM(stream.shape, BF16)] * 2,
                *[blocks[0] for mask, blocks in late], held_out, partial, *kept,
            )
        return call(
            lambda *refs: out_kernel(late_masks, keep_section, *refs),
            [VMEM(stream.shape, BF16)],
            *[blocks[0] for mask, blocks in late], held_out, partial, stream if kept is None else kept,
        )[0]

    def layer(stream, others, parts, keep_section=None, kept=None, section=None):
        mix = attend(others, parts)
        mixes = from_peers(mix, section=section)
        return project(mixes, mix, stream, keep_section, kept)

    def handed_on(out, far):
        own = crossed(out, 0, 0)
        others = [(FAR, (crossed(far, FAR, 0),))]
        others += [(mask, (swapped(own, mask, 1),)) for mask in REST_ORDER]
        return own, others

    def rotated(x, by):
        return lax.ppermute(x, "section", [(i, (i + by) % sections) for i in range(sections)])

    if sections == 2 and peers == MOST_DIRECT:
        others = [
            (mask, (swapped(raw, mask, 0 if mask in (3,) else None),))
            for mask in FIRST_ORDER
        ]
        ahead = crossed(raw, 3, 1)
        stream, gain, held_qkv, *parts, bias = load()
        held_out = fetch(weights_out)
        far = dict(others)[FAR][0]
        out, far = layer(stream, others, parts, None, (stream, far))
        stream, others = handed_on(out, far)
        others = [(mask, (ahead, *blocks) if mask == 3 else blocks) for mask, blocks in others]
        stream, parts = add_own((stream,))
        out = layer(stream, others, parts)
        finished, others = handed_on(out, out)
        stream, parts = add_own((finished,))
        return layer(stream, others, parts, 0, finished)[None]
    others = from_peers(raw, FIRST_ORDER)
    current, gain, held_qkv, *parts, bias = load()
    held_out = fetch(weights_out)
    ticks = 2 * sections - 1
    result = current
    for tick in range(ticks):
        if tick + 1 < sections:
            raw = rotated(raw, -1)
        out = layer(current, others, parts)
        done = tick - (sections - 1)
        if tick + 1 < ticks:
            sent = rotated(out, 1)
            current = pick(0, raw, sent)
            others = from_peers(current)
            current, parts = add_own((current,))
        if done >= 0:
            owned = rotated(out, done + 1) if done + 1 < sections else out
            result = pick(done, owned, result)
    return result[None]


def solution(mesh):
    in_specs = (
        P(("dp", "section"), None, "mp"),
        P("section", None, None, "mp"),
        P("section", None, "mp"),
        P("section", None),
        P("mp", None),
    )
    out_specs = P(("dp", "section"), None, "mp")
    return jax.shard_map(shards, mesh=mesh, in_specs=in_specs, out_specs=out_specs, check_vma=False)
```
